32 devices in a mesh: dp: 8 (over z, x), tensor: 4 (over y, core).
Axes of the slice: x: 2, y: 2, z: 4, core: 2. Of those that a mesh axis runs over, the one named last changes fastest.
Arguments:
- hidden_in: bfloat16 [32, 128, 4096], P(('dp', 'tensor')), parts along dimension 0, may hold values from -6 to 6
- norm_gain: float32 [4096], replicated, may hold values from 0.1 to 1.9
- query_weight: bfloat16 [4096, 4096], P(None, 'tensor'), may hold values from -3 to 3
- kv_weight: bfloat16 [4096, 2048], P(None, 'tensor'), may hold values from -3 to 3
- output_weight: bfloat16 [4096, 4096], P('tensor'), may hold values from -0.09375 to 0.09375
Outputs:
- attention_out: bfloat16 [32, 128, 4096], P(('dp', 'tensor')), parts along dimension 0
The draws below stay inside these ranges and needn't reach their ends.
There are 8 independent parts, one for each index of `dp`. The reference program is written for one: setup_inputs(seed, part) draws one part's arguments, and reference() takes and returns one part's arrays. A program takes and returns all parts, laid end to end along the dimension named above; an argument that names none is the same for every part. Nothing has to cross between parts.
All inputs are finite; a program needn't handle non-finite values.
Results may differ from the reference program's by a relative error of at most 0.014.
The reference program's roundings to bfloat16 on the way (of `normed`, `probabilities` and `mixed`) count: a program that leaves them out, or rounds other values in their place, can miss the bound.
Values may be sent and summed in bfloat16 or wider, within the bound.
A program may use at most 128 MiB of HBM per device.

```python
import math
import jax
import jax.numpy as jnp
from jax import lax

D = 4096
H = 32
KVH = 8
HD = 128
SEQ_LEN = 128
SEQS = 4


def projection_base(key):
    base = jnp.clip(jax.random.normal(jax.random.fold_in(key, 11), (D, H * HD), jnp.float32), -4.0, 4.0)
    return base


def draw_query_weight(key, part):
    base = projection_base(key)
    return (base * D ** (-0.5)).astype(jnp.bfloat16)


def draw_kv_weight(key, part):
    own_part = jnp.clip(jax.random.normal(jax.random.fold_in(key, 13), (D, KVH * HD), jnp.float32), -4.0, 4.0)
    value_part = jnp.clip(jax.random.normal(jax.random.fold_in(key, 14), (D, KVH * HD), jnp.float32), -4.0, 4.0)
    key_part = own_part
    joined = jnp.stack((key_part.reshape(D, KVH, HD), value_part.reshape(D, KVH, HD)), axis=2)
    return (joined.reshape(D, 2 * KVH * HD) * D ** (-0.5)).astype(jnp.bfloat16)


def block_levels(key, shape, cuts, smallest, largest):
    gain = 1.0
    for axis_at, blocks in cuts:
        heights = jax.random.uniform(jax.random.fold_in(jax.random.fold_in(key, 6), axis_at), (blocks,), jnp.float32, smallest / len(cuts), largest / len(cuts))
        gain = gain * jnp.repeat(jnp.exp(heights), shape[axis_at] // blocks).reshape((-1,) + (1,) * (len(shape) - 1 - axis_at))
    return gain


def noise(rng, dims, spread, most, shards=(), held_as=jnp.bfloat16):
    values = spread * jax.random.normal(rng, dims, jnp.float32)
    if shards:
        values = values * block_levels(rng, dims, shards, -0.22, 0.18)
    return jnp.clip(values, -most, most).astype(held_as)


def setup_inputs(seed: int = 0, part: int = 0) -> dict:
    seeds = jax.random.split(jax.random.key(seed), 6)
    own_keys = jax.random.split(jax.random.fold_in(seeds[5], part), 6)
    hidden_in = noise(own_keys[0], (SEQS, SEQ_LEN, D), 1.0, 6.0, ((0, 4),))
    norm_gain = jnp.clip(1.0 + 0.18 * jax.random.normal(seeds[1], (D,), jnp.float32), 0.1, 1.9)
    query_weight = draw_query_weight(jax.random.fold_in(seeds[5], 71), part)
    kv_weight = draw_kv_weight(jax.random.fold_in(seeds[5], 71), part)
    output_weight = noise(seeds[4], (H * HD, D), (H * HD) ** -0.5, 0.09375, ((0, 4),))
    return {"hidden_in": hidden_in, "norm_gain": norm_gain, "query_weight": query_weight, "kv_weight": kv_weight, "output_weight": output_weight}


EPS = 1e-05
THETA = 500000.0

def rotary(tensor, positions):
    half_width = tensor.shape[-1] // 2
    frequency = THETA ** (-(jnp.arange(half_width, dtype=jnp.float32) * 2.0 / tensor.shape[-1]))
    angles = positions[:, None] * frequency[None, :]
    cosine = jnp.cos(angles)[:, None, :]
    sine_part = jnp.sin(angles)[:, None, :]
    first_half = tensor[..., :half_width]
    second_half = tensor[..., half_width:]
    return jnp.concatenate((first_half * cosine - second_half * sine_part, second_half * cosine + first_half * sine_part), axis=-1)

def rms_norm(hidden_in, norm_gain):
    wide = hidden_in.astype(jnp.float32)
    mean_square = lax.optimization_barrier(jnp.mean(wide * wide, axis=-1, keepdims=True))
    return (wide * lax.rsqrt(mean_square + EPS) * norm_gain).astype(jnp.bfloat16)

def attend(queries, keys, values):
    length = queries.shape[1]
    scores = jnp.einsum('bqhgd,bkhd->bhgqk', queries.astype(jnp.float32), keys.astype(jnp.float32)) / math.sqrt(queries.shape[-1])
    causal = jnp.arange(length)[:, None] >= jnp.arange(length)[None, :]
    scores = jnp.where(causal, scores, -1e+30)
    highest = lax.optimization_barrier(jnp.max(scores, axis=-1, keepdims=True))
    exponent = jnp.exp(scores - highest)
    probabilities = (exponent / lax.optimization_barrier(jnp.sum(exponent, axis=-1, keepdims=True))).astype(jnp.bfloat16)
    mixed = jnp.einsum('bhgqk,bkhd->bqhgd', probabilities.astype(jnp.float32), values.astype(jnp.float32))
    return mixed.astype(jnp.bfloat16)

def reference(hidden_in, norm_gain, query_weight, kv_weight, output_weight):
    normed = rms_norm(hidden_in, norm_gain).astype(jnp.float32)
    queries_raw = jnp.einsum('bld,dc->blc', normed, query_weight.astype(jnp.float32))
    kv_raw = jnp.einsum('bld,dc->blc', normed, kv_weight.astype(jnp.float32)).astype(jnp.bfloat16)
    kv_split = kv_raw.reshape(SEQS, SEQ_LEN, KVH, 2, HD)
    keys_raw = kv_split[:, :, :, 0, :]
    values = kv_split[:, :, :, 1, :]
    positions = jnp.arange(SEQ_LEN, dtype=jnp.float32)
    queries = rotary(queries_raw.reshape(SEQS, SEQ_LEN, H, HD), positions).astype(jnp.bfloat16)
    keys_wide = lax.optimization_barrier(keys_raw).astype(jnp.float32)
    keys = rotary(keys_wide, positions).astype(jnp.bfloat16)
    mixed = attend(queries.reshape(SEQS, SEQ_LEN, KVH, H // KVH, HD), keys, values)
    result = jnp.einsum('blc,cd->bld', mixed.reshape(SEQS, SEQ_LEN, H * HD).astype(jnp.float32), output_weight.astype(jnp.float32))
    return result.astype(jnp.bfloat16)
```

```python
import functools
import math

import jax
import jax.numpy as jnp
from jax import lax
import numpy as np
from jax.experimental import pallas as pl
from jax.experimental.pallas import tpu as pltpu
from jax.sharding import PartitionSpec as P

KVH = 8
HD = 128


EPS = 1e-05
THETA = 500000.0


def partner_2(value, axis, bit):
    mask = 2**bit
    pairs = [(source, source ^ mask) for source in range(lax.axis_size(axis))]
    return lax.ppermute(value, axis, pairs)


def rotary(tensor, positions):
    half_width = tensor.shape[-1] // 2
    frequency = THETA ** (-(jnp.arange(half_width, dtype=jnp.float32) * 2.0 / tensor.shape[-1]))
    angles = positions[:, None] * frequency[None, :]
    cosine = jnp.cos(angles)[:, None, :]
    sine_part = jnp.sin(angles)[:, None, :]
    first_half = tensor[..., :half_width]
    second_half = tensor[..., half_width:]
    return jnp.concatenate(
        (
            first_half * cosine - second_half * sine_part,
            second_half * cosine + first_half * sine_part,
        ),
        axis=-1,
    )


def rms_norm(hidden_in, norm_gain):
    wide = hidden_in.astype(jnp.float32)
    mean_square = jnp.mean(wide * wide, axis=-1, keepdims=True)
    return (wide * lax.rsqrt(mean_square + EPS) * norm_gain).astype(jnp.bfloat16)


def attend(queries, keys, values):
    length = queries.shape[1]
    scores = jnp.einsum(
        "bqhgd,bkhd->bhgqk", queries, keys, preferred_element_type=jnp.float32
    ) / math.sqrt(queries.shape[-1])
    causal = jnp.arange(length)[:, None] >= jnp.arange(length)[None, :]
    scores = jnp.where(causal, scores, -1e30)
    highest = jnp.max(scores, axis=-1, keepdims=True)
    exponent = jnp.exp(scores - highest)
    probabilities = (exponent / jnp.sum(exponent, axis=-1, keepdims=True)).astype(jnp.bfloat16)
    mixed = jnp.einsum(
        "bhgqk,bkhd->bqhgd", probabilities, values, preferred_element_type=jnp.float32
    )
    return mixed.astype(jnp.bfloat16)


def join_heads(stacked, axis_dim):
    sharers = max(lax.axis_size("tensor") // KVH, 1)
    position = lax.axis_index("tensor")
    for bit_index in range(sharers.bit_length() - 1):
        partner = partner_2(stacked, "tensor", bit_index)
        keeps_first = position // (1 << bit_index) % 2 == 0
        stacked = jnp.where(
            keeps_first,
            jnp.concatenate((stacked, partner), axis_dim),
            jnp.concatenate((partner, stacked), axis_dim),
        )
    return stacked


def general_shards(hidden_in, norm_gain, query_weight, kv_weight, output_weight):
    merged_weight = jnp.concatenate((query_weight, kv_weight), axis=1)
    query_cols = query_weight.shape[1]
    normed = rms_norm(hidden_in, norm_gain)
    projected = jnp.einsum(
        "brd,dc->brc",
        lax.all_gather(normed, "tensor", axis=0, tiled=True),
        merged_weight,
        preferred_element_type=jnp.float32,
    )
    batch, length = (projected.shape[0], projected.shape[1])
    queries_raw = projected[..., :query_cols]
    kv_raw = projected[..., query_cols:].astype(jnp.bfloat16)
    kv_raw = join_heads(kv_raw, 2)
    kv_heads = kv_raw.shape[-1] // (2 * HD)
    kv_split = kv_raw.reshape(batch, length, kv_heads, 2, HD)
    keys_raw = kv_split[:, :, :, 0, :]
    values = kv_split[:, :, :, 1, :]
    heads = query_cols // HD
    positions = jnp.arange(length, dtype=jnp.float32)
    queries = rotary(queries_raw.reshape(batch, length, heads, HD), positions).astype(jnp.bfloat16)
    keys = rotary(keys_raw.astype(jnp.float32), positions).astype(jnp.bfloat16)
    mixed = attend(queries.reshape(batch, length, kv_heads, heads // kv_heads, HD), keys, values)
    mixed_rows = mixed.reshape(batch, length, heads * HD)
    partial_out = jnp.einsum(
        "blc,cd->bld", mixed_rows, output_weight, preferred_element_type=jnp.float32
    )
    return lax.psum_scatter(
        partial_out.astype(jnp.bfloat16), "tensor", scatter_dimension=0, tiled=True
    )


MESH = pl.DeviceIdType.MESH
CORES = 2
HALVES = 2
LAG = 3
OUT_TILES = 8


def rotary_tables(length):
    half = HD // 2
    frequency = np.float32(THETA) ** (-(np.arange(half, dtype=np.float32) * np.float32(2.0 / HD)))
    angles = np.arange(length, dtype=np.float32)[:, None] * frequency[None, :].astype(np.float32)
    cosine, sine = np.cos(angles), np.sin(angles)
    return (
        np.concatenate((cosine, cosine), axis=1).astype(np.float32),
        np.concatenate((-sine, sine), axis=1).astype(np.float32),
    )


def block_kernel(
    dims,
    hid, gain, wq, wkv, wo, cosine, sine,
    out,
    x, xn, w1, w2, qs, ks, vs, mixed_own, mixed_far,
    give, got, held, summed, landed, own_acc, own_give, own_got, out_buf,
    x_sem, w1_sem, w2_sem, sib_send, sib_recv, far_send, far_recv, fwd_send, fwd_recv,
    give_send, give_recv, sum_send, sum_recv, own_send, own_recv, out_sem,
):
    length, kvh, group, q_tiles, o_width = dims
    part = length // HALVES
    me = lax.axis_index("tensor")
    sibling = me + 1 - 2 * lax.rem(me, CORES)
    across = lax.rem(me + CORES, 2 * CORES)

    def local_copy(src, dst, sem):
        return pltpu.make_async_copy(src, dst, sem)

    def remote(src, dst, send, recv, target):
        return pltpu.make_async_remote_copy(
            src_ref=src, dst_ref=dst, send_sem=send, recv_sem=recv,
            device_id={"tensor": target}, device_id_type=MESH,
        )

    def w1_copy(t, kv):
        cols = pl.ds(pl.multiple_of(t * 2 * HD, 2 * HD), 2 * HD)
        if kv:
            return local_copy(wkv.at[:, cols], w1.at[t], w1_sem.at[t])
        return local_copy(wq.at[:, cols], w1.at[kvh + t], w1_sem.at[kvh + t])

    def w2_copy(j):
        cols = pl.ds(pl.multiple_of(j * o_width, o_width), o_width)
        return local_copy(wo.at[:, cols], w2.at[j], w2_sem.at[j])

    def far_copy(h):
        rows = pl.ds(h * part, part)
        return remote(hid.at[0, rows], x.at[2, rows], far_send.at[h], far_recv.at[h], across)

    def fwd_copy(h):
        rows = pl.ds(h * part, part)
        return remote(x.at[2, rows], x.at[3, rows], fwd_send.at[h], fwd_recv.at[h], sibling)

    def give_copy(h, j):
        return remote(give.at[h, j], got.at[h, j], give_send.at[h, j], give_recv.at[h, j], sibling)

    def sum_copy(h, j):
        return remote(summed.at[h, j], landed.at[h, j], sum_send.at[h, j], sum_recv.at[h, j], across)

    def own_copy(j):
        return remote(own_give.at[j], own_got.at[j], own_send.at[j], own_recv.at[j], sibling)

    def out_copy(j):
        cols = pl.ds(pl.multiple_of(j * o_width, o_width), o_width)
        return local_copy(out_buf.at[j], out.at[0, :, cols], out_sem.at[j])

    x_copy = local_copy(hid.at[0], x.at[0], x_sem)
    sib_copy = remote(hid.at[0], x.at[1], sib_send, sib_recv, sibling)

    x_copy.start()
    for t in range(kvh):
        w1_copy(t, True).start()
    for t in range(q_tiles):
        w1_copy(t, False).start()
    for j in range(OUT_TILES):
        w2_copy(j).start()

    barrier = pltpu.get_barrier_semaphore()
    for target in (sibling, across):
        pl.semaphore_signal(barrier, inc=1, device_id={"tensor": target}, device_id_type=MESH)
    pl.semaphore_wait(barrier, 2)

    sib_copy.start()
    for h in range(HALVES):
        far_copy(h).start()

    def normalise(slot, row0, rows, dst0):
        step = 16

        def body(i, carry):
            at = pl.multiple_of(i * step, step)
            wide = x[slot, pl.ds(row0 + at, step), :].astype(jnp.float32)
            mean_square = jnp.mean(wide * wide, axis=-1, keepdims=True)
            scaled = wide * lax.rsqrt(mean_square + EPS) * gain[...]
            xn[pl.ds(dst0 + at, step), :] = scaled.astype(jnp.bfloat16)
            return carry

        lax.fori_loop(0, rows // step, body, 0)

    def rotate(value, row0, rows):
        c = cosine[row0 : row0 + rows, :]
        s = sine[row0 : row0 + rows, :]
        return value * c + pltpu.roll(value, HD // 2, 1) * s

    def project(slot0, row0, rows, first):
        both = 2 * rows

        def kv_body(g, carry):
            if first:
                w1_copy(g, True).wait()
            raw = jnp.dot(xn[:both, :], w1[g], preferred_element_type=jnp.float32).astype(jnp.bfloat16)
            for s in range(2):
                mine = raw[s * rows : (s + 1) * rows]
                keys = rotate(mine[:, :HD].astype(jnp.float32), row0, rows)
                ks[slot0 + s, g, row0 : row0 + rows, :] = keys.astype(jnp.bfloat16)
                vs[slot0 + s, g, row0 : row0 + rows, :] = mine[:, HD:]
            return carry

        def q_body(t, carry):
            if first:
                w1_copy(t, False).wait()
            raw = jnp.dot(xn[:both, :], w1[kvh + t], preferred_element_type=jnp.float32)
            for s in range(2):
                for e in range(2):
                    value = raw[s * rows : (s + 1) * rows, e * HD : (e + 1) * HD]
                    qs[s, 2 * t + e, :rows, :] = rotate(value, row0, rows).astype(jnp.bfloat16)
            return carry

        lax.fori_loop(0, kvh, kv_body, 0)
        lax.fori_loop(0, q_tiles, q_body, 0)

    def attention(slot0, row0, rows, mixed):
        seen = row0 + rows
        for s in range(2):
            for g in range(kvh):
                queries = qs[s, g * group : (g + 1) * group, :rows, :].reshape(group * rows, HD)
                keys = ks[slot0 + s, g, :seen, :]
                scores = lax.dot_general(
                    queries, keys, (((1,), (1,)), ((), ())), preferred_element_type=jnp.float32
                ) * (1.0 / math.sqrt(HD))
                scores = scores.reshape(group, rows, seen)
                position = row0 + lax.broadcasted_iota(jnp.int32, (group, rows, seen), 1)
                key_at = lax.broadcasted_iota(jnp.int32, (group, rows, seen), 2)
                scores = jnp.where(position >= key_at, scores, -1e30)
                highest = jnp.max(scores, axis=-1, keepdims=True)
                exponent = jnp.exp(scores - highest)
                total = jnp.sum(exponent, axis=-1, keepdims=True)
                probabilities = (exponent * (1.0 / total)).astype(jnp.bfloat16)
                result = jnp.dot(
                    probabilities.reshape(group * rows, seen),
                    vs[slot0 + s, g, :seen, :],
                    preferred_element_type=jnp.float32,
                ).astype(jnp.bfloat16)
                for e in range(group):
                    head = g * group + e
                    mixed[s * rows : (s + 1) * rows, head * HD : (head + 1) * HD] = result[
                        e * rows : (e + 1) * rows
                    ]

    x_copy.wait()
    normalise(0, 0, length, 0)
    sib_copy.wait_recv()
    normalise(1, 0, length, length)
    project(0, 0, length, True)
    attention(0, 0, length, mixed_own)

    for h in range(HALVES):
        row0 = h * part
        far_copy(h).wait_recv()
        fwd_copy(h).start()
        normalise(2, row0, part, 0)
        fwd_copy(h).wait_recv()
        normalise(3, row0, part, part)
        project(2, row0, part, False)
        attention(2, row0, part, mixed_far)

        def far_out(j, carry, h=h):
            @pl.when(j < OUT_TILES)
            def _():
                if h == 0:
                    w2_copy(j).wait()
                partial = jnp.dot(mixed_far[...], w2[j], preferred_element_type=jnp.float32)
                held[j] = partial[:part]
                give[h, j] = partial[part:].astype(jnp.bfloat16)
                give_copy(h, j).start()

            @pl.when(j >= LAG)
            def _():
                t = j - LAG
                give_copy(h, t).wait_recv()
                summed[h, t] = (held[t] + got[h, t].astype(jnp.float32)).astype(jnp.bfloat16)
                sum_copy(h, t).start()

            return carry

        lax.fori_loop(0, OUT_TILES + LAG, far_out, 0)

    def own_out(j, carry):
        partial = jnp.dot(mixed_own[...], w2[j], preferred_element_type=jnp.float32)
        own_acc[j] = partial[:length]
        own_give[j] = partial[length:].astype(jnp.bfloat16)
        own_copy(j).start()
        return carry

    lax.fori_loop(0, OUT_TILES, own_out, 0)

    for h in range(HALVES):

        def finish(j, carry, h=h):
            rows = pl.ds(h * part, part)
            if h == 0:
                own_copy(j).wait_recv()
            sum_copy(h, j).wait_recv()
            out_buf[j, rows, :] = (
                own_acc[j, rows, :] + own_got[j, rows, :].astype(jnp.float32)
                + landed[h, j].astype(jnp.float32)
            ).astype(jnp.bfloat16)
            if h == HALVES - 1:
                out_copy(j).start()
            return carry

        lax.fori_loop(0, OUT_TILES, finish, 0)

    def drain(j, carry):
        out_copy(j).wait()
        own_copy(j).wait_send()
        for h in range(HALVES):
            give_copy(h, j).wait_send()
            sum_copy(h, j).wait_send()
        return carry

    lax.fori_loop(0, OUT_TILES, drain, 0)
    sib_copy.wait_send()
    for h in range(HALVES):
        far_copy(h).wait_send()
        fwd_copy(h).wait_send()


def paired_shards(hidden_in, norm_gain, query_weight, kv_weight, output_weight):
    _, length, width = hidden_in.shape
    query_cols, kv_cols = query_weight.shape[1], kv_weight.shape[1]
    heads, kvh = query_cols // HD, kv_cols // (2 * HD)
    q_tiles = query_cols // (2 * HD)
    part = length // HALVES
    o_width = width // OUT_TILES
    cosine, sine = rotary_tables(length)
    bf16, f32 = jnp.bfloat16, jnp.float32
    dma = pltpu.SemaphoreType.DMA
    any_spec = pl.BlockSpec(memory_space=pl.ANY)
    vmem_spec = pl.BlockSpec(memory_space=pltpu.VMEM)
    dims = (length, kvh, heads // kvh, q_tiles, o_width)
    return pl.pallas_call(
        functools.partial(block_kernel, dims),
        out_shape=jax.ShapeDtypeStruct(hidden_in.shape, bf16),
        in_specs=[any_spec, vmem_spec, any_spec, any_spec, any_spec, vmem_spec, vmem_spec],
        out_specs=any_spec,
        scratch_shapes=[
            pltpu.VMEM((4, length, width), bf16),
            pltpu.VMEM((2 * length, width), bf16),
            pltpu.VMEM((kvh + q_tiles, width, 2 * HD), bf16),
            pltpu.VMEM((OUT_TILES, query_cols, o_width), bf16),
            pltpu.VMEM((2, heads, length, HD), bf16),
            pltpu.VMEM((4, kvh, length, HD), bf16),
            pltpu.VMEM((4, kvh, length, HD), bf16),
            pltpu.VMEM((2 * length, query_cols), bf16),
            pltpu.VMEM((2 * part, query_cols), bf16),
            pltpu.VMEM((HALVES, OUT_TILES, part, o_width), bf16),
            pltpu.VMEM((HALVES, OUT_TILES, part, o_width), bf16),
            pltpu.VMEM((OUT_TILES, part, o_width), f32),
            pltpu.VMEM((HALVES, OUT_TILES, part, o_width), bf16),
            pltpu.VMEM((HALVES, OUT_TILES, part, o_width), bf16),
            pltpu.VMEM((OUT_TILES, length, o_width), f32),
            pltpu.VMEM((OUT_TILES, length, o_width), bf16),
            pltpu.VMEM((OUT_TILES, length, o_width), bf16),
            pltpu.VMEM((OUT_TILES, length, o_width), bf16),
            dma,
            dma((kvh + q_tiles,)),
            dma((OUT_TILES,)),
            dma, dma,
            dma((HALVES,)), dma((HALVES,)),
            dma((HALVES,)), dma((HALVES,)),
            dma((HALVES, OUT_TILES)), dma((HALVES, OUT_TILES)),
            dma((HALVES, OUT_TILES)), dma((HALVES, OUT_TILES)),
            dma((OUT_TILES,)), dma((OUT_TILES,)),
            dma((OUT_TILES,)),
        ],
        compiler_params=pltpu.CompilerParams(
            collective_id=0, has_side_effects=True, vmem_limit_bytes=60 * 2**20
        ),
    )(
        hidden_in, norm_gain.reshape(1, width), query_weight, kv_weight, output_weight,
        jnp.asarray(cosine), jnp.asarray(sine),
    )


def shards(hidden_in, norm_gain, query_weight, kv_weight, output_weight):
    two_chips = lax.axis_size("tensor") == 2 * CORES
    whole_heads = kv_weight.shape[1] % (2 * HD) == 0
    if two_chips and whole_heads and hidden_in.shape[0] == 1:
        return paired_shards(hidden_in, norm_gain, query_weight, kv_weight, output_weight)
    return general_shards(hidden_in, norm_gain, query_weight, kv_weight, output_weight)


def solution(mesh):
    placed = (
        P(("dp", "tensor"), None, None),
        P(),
        P(None, "tensor"),
        P(None, "tensor"),
        P("tensor", None),
    )
    return jax.shard_map(
        shards,
        mesh=mesh,
        in_specs=placed,
        out_specs=P(("dp", "tensor"), None, None),
        check_vma=False,
    )
```

```python
import functools
import math

import jax
import jax.numpy as jnp
from jax import lax
import numpy as np
from jax.experimental import pallas as pl
from jax.experimental.pallas import tpu as pltpu
from jax.sharding import PartitionSpec as P

KVH = 8
HD = 128


EPS = 1e-05
THETA = 500000.0


def partner_2(value, axis, bit):
    mask = 2**bit
    pairs = [(source, source ^ mask) for source in range(lax.axis_size(axis))]
    return lax.ppermute(value, axis, pairs)


def rotary(tensor, positions):
    half_width = tensor.shape[-1] // 2
    frequency = THETA ** (-(jnp.arange(half_width, dtype=jnp.float32) * 2.0 / tensor.shape[-1]))
    angles = positions[:, None] * frequency[None, :]
    cosine = jnp.cos(angles)[:, None, :]
    sine_part = jnp.sin(angles)[:, None, :]
    first_half = tensor[..., :half_width]
    second_half = tensor[..., half_width:]
    return jnp.concatenate(
        (
            first_half * cosine - second_half * sine_part,
            second_half * cosine + first_half * sine_part,
        ),
        axis=-1,
    )


def rms_norm(hidden_in, norm_gain):
    wide = hidden_in.astype(jnp.float32)
    mean_square = jnp.mean(wide * wide, axis=-1, keepdims=True)
    return (wide * lax.rsqrt(mean_square + EPS) * norm_gain).astype(jnp.bfloat16)


def attend(queries, keys, values):
    length = queries.shape[1]
    scores = jnp.einsum(
        "bqhgd,bkhd->bhgqk", queries, keys, preferred_element_type=jnp.float32
    ) / math.sqrt(queries.shape[-1])
    causal = jnp.arange(length)[:, None] >= jnp.arange(length)[None, :]
    scores = jnp.where(causal, scores, -1e30)
    highest = jnp.max(scores, axis=-1, keepdims=True)
    exponent = jnp.exp(scores - highest)
    probabilities = (exponent / jnp.sum(exponent, axis=-1, keepdims=True)).astype(jnp.bfloat16)
    mixed = jnp.einsum(
        "bhgqk,bkhd->bqhgd", probabilities, values, preferred_element_type=jnp.float32
    )
    return mixed.astype(jnp.bfloat16)


def join_heads(stacked, axis_dim):
    sharers = max(lax.axis_size("tensor") // KVH, 1)
    position = lax.axis_index("tensor")
    for bit_index in range(sharers.bit_length() - 1):
        partner = partner_2(stacked, "tensor", bit_index)
        keeps_first = position // (1 << bit_index) % 2 == 0
        stacked = jnp.where(
            keeps_first,
            jnp.concatenate((stacked, partner), axis_dim),
            jnp.concatenate((partner, stacked), axis_dim),
        )
    return stacked


def general_shards(hidden_in, norm_gain, query_weight, kv_weight, output_weight):
    merged_weight = jnp.concatenate((query_weight, kv_weight), axis=1)
    query_cols = query_weight.shape[1]
    normed = rms_norm(hidden_in, norm_gain)
    projected = jnp.einsum(
        "brd,dc->brc",
        lax.all_gather(normed, "tensor", axis=0, tiled=True),
        merged_weight,
        preferred_element_type=jnp.float32,
    )
    batch, length = (projected.shape[0], projected.shape[1])
    queries_raw = projected[..., :query_cols]
    kv_raw = projected[..., query_cols:].astype(jnp.bfloat16)
    kv_raw = join_heads(kv_raw, 2)
    kv_heads = kv_raw.shape[-1] // (2 * HD)
    kv_split = kv_raw.reshape(batch, length, kv_heads, 2, HD)
    keys_raw = kv_split[:, :, :, 0, :]
    values = kv_split[:, :, :, 1, :]
    heads = query_cols // HD
    positions = jnp.arange(length, dtype=jnp.float32)
    queries = rotary(queries_raw.reshape(batch, length, heads, HD), positions).astype(jnp.bfloat16)
    keys = rotary(keys_raw.astype(jnp.float32), positions).astype(jnp.bfloat16)
    mixed = attend(queries.reshape(batch, length, kv_heads, heads // kv_heads, HD), keys, values)
    mixed_rows = mixed.reshape(batch, length, heads * HD)
    partial_out = jnp.einsum(
        "blc,cd->bld", mixed_rows, output_weight, preferred_element_type=jnp.float32
    )
    return lax.psum_scatter(
        partial_out.astype(jnp.bfloat16), "tensor", scatter_dimension=0, tiled=True
    )


MESH = pl.DeviceIdType.MESH
CORES = 2
HALVES = 2
LAG = 3
OUT_TILES = 8


def rotary_tables(length):
    half = HD // 2
    frequency = np.float32(THETA) ** (-(np.arange(half, dtype=np.float32) * np.float32(2.0 / HD)))
    angles = np.arange(length, dtype=np.float32)[:, None] * frequency[None, :].astype(np.float32)
    cosine, sine = np.cos(angles), np.sin(angles)
    return (
        np.concatenate((cosine, cosine), axis=1).astype(np.float32),
        np.concatenate((-sine, sine), axis=1).astype(np.float32),
    )


def block_kernel(
    dims,
    hid, gain_in, wq, wkv, wo, cosine_in, sine_in,
    out,
    gain, cosine, sine,
    x, xn, w1, w2, qs, ks, vs, mixed_own, mixed_far,
    give, got, held, summed, landed, own_acc, own_give, own_got,
    x_sem, w1_sem, w2_sem, sib_send, sib_recv, far_send, far_recv, fwd_send, fwd_recv,
    give_send, give_recv, sum_send, sum_recv, own_send, own_recv, table_sem,
):
    length, kvh, group, q_tiles, o_width = dims
    part = length // HALVES
    me = lax.axis_index("tensor")
    sibling = me + 1 - 2 * lax.rem(me, CORES)
    across = lax.rem(me + CORES, 2 * CORES)

    def local_copy(src, dst, sem):
        return pltpu.make_async_copy(src, dst, sem)

    def remote(src, dst, send, recv, target):
        return pltpu.make_async_remote_copy(
            src_ref=src, dst_ref=dst, send_sem=send, recv_sem=recv,
            device_id={"tensor": target}, device_id_type=MESH,
        )

    def w1_copy(t, kv):
        cols = pl.ds(pl.multiple_of(t * 2 * HD, 2 * HD), 2 * HD)
        if kv:
            return local_copy(wkv.at[:, cols], w1.at[t], w1_sem.at[t])
        return local_copy(wq.at[:, cols], w1.at[kvh + t], w1_sem.at[kvh + t])

    def w2_copy(j):
        cols = pl.ds(pl.multiple_of(j * o_width, o_width), o_width)
        return local_copy(wo.at[:, cols], w2.at[j], w2_sem.at[j])

    def far_copy(h):
        rows = pl.ds(h * part, part)
        return remote(hid.at[0, rows], x.at[2, rows], far_send.at[h], far_recv.at[h], across)

    def fwd_copy(h):
        rows = pl.ds(h * part, part)
        return remote(x.at[2, rows], x.at[3, rows], fwd_send.at[h], fwd_recv.at[h], sibling)

    def give_copy(h, j):
        return remote(give.at[h, j], got.at[h, j], give_send.at[h, j], give_recv.at[h, j], sibling)

    def sum_copy(h, j):
        return remote(summed.at[h, j], landed.at[h, j], sum_send.at[h, j], sum_recv.at[h, j], across)

    def own_copy(j):
        return remote(own_give.at[j], own_got.at[j], own_send.at[j], own_recv.at[j], sibling)

    x_copy = local_copy(hid.at[0], x.at[0], x_sem)
    sib_copy = remote(hid.at[0], x.at[1], sib_send, sib_recv, sibling)

    tables = [
        local_copy(src, dst, table_sem.at[i])
        for i, (src, dst) in enumerate(((gain_in, gain), (cosine_in, cosine), (sine_in, sine)))
    ]
    barrier = pltpu.get_barrier_semaphore()
    for target in (sibling, across):
        pl.semaphore_signal(barrier, inc=1, device_id={"tensor": target}, device_id_type=MESH)

    x_copy.start()
    for table in tables:
        table.start()
    for t in range(kvh):
        w1_copy(t, True).start()
    for t in range(q_tiles):
        w1_copy(t, False).start()
    for j in range(OUT_TILES):
        w2_copy(j).start()

    pl.semaphore_wait(barrier, 2)
    for h in range(HALVES):
        far_copy(h).start()
    sib_copy.start()

    def normalise(slot, row0, rows, dst0):
        step = 16

        def body(i, carry):
            at = pl.multiple_of(i * step, step)
            wide = x[slot, pl.ds(row0 + at, step), :].astype(jnp.float32)
            mean_square = jnp.mean(wide * wide, axis=-1, keepdims=True)
            scaled = wide * lax.rsqrt(mean_square + EPS) * gain[...]
            xn[pl.ds(dst0 + at, step), :] = scaled.astype(jnp.bfloat16)
            return carry

        lax.fori_loop(0, rows // step, body, 0)

    def rotate(value, row0, rows):
        c = cosine[row0 : row0 + rows, :]
        s = sine[row0 : row0 + rows, :]
        return value * c + pltpu.roll(value, HD // 2, 1) * s

    def project(slot0, row0, rows, first):
        both = 2 * rows

        def kv_body(g, carry):
            if first:
                w1_copy(g, True).wait()
            raw = jnp.dot(xn[:both, :], w1[g], preferred_element_type=jnp.float32).astype(jnp.bfloat16)
            for s in range(2):
                mine = raw[s * rows : (s + 1) * rows]
                keys = rotate(mine[:, :HD].astype(jnp.float32), row0, rows)
                ks[slot0 + s, g, row0 : row0 + rows, :] = keys.astype(jnp.bfloat16)
                vs[slot0 + s, g, row0 : row0 + rows, :] = mine[:, HD:]
            return carry

        def q_body(t, carry):
            if first:
                w1_copy(t, False).wait()
            raw = jnp.dot(xn[:both, :], w1[kvh + t], preferred_element_type=jnp.float32)
            for s in range(2):
                for e in range(2):
                    value = raw[s * rows : (s + 1) * rows, e * HD : (e + 1) * HD]
                    qs[s, 2 * t + e, :rows, :] = rotate(value, row0, rows).astype(jnp.bfloat16)
            return carry

        lax.fori_loop(0, kvh, kv_body, 0)
        lax.fori_loop(0, q_tiles, q_body, 0)

    def attention(slot0, row0, rows, mixed):
        seen = row0 + rows
        for s in range(2):
            for g in range(kvh):
                queries = qs[s, g * group : (g + 1) * group, :rows, :].reshape(group * rows, HD)
                keys = ks[slot0 + s, g, :seen, :]
                scores = lax.dot_general(
                    queries, keys, (((1,), (1,)), ((), ())), preferred_element_type=jnp.float32
                ) * (1.0 / math.sqrt(HD))
                scores = scores.reshape(group, rows, seen)
                position = row0 + lax.broadcasted_iota(jnp.int32, (group, rows, seen), 1)
                key_at = lax.broadcasted_iota(jnp.int32, (group, rows, seen), 2)
                scores = jnp.where(position >= key_at, scores, -1e30)
                highest = jnp.max(scores, axis=-1, keepdims=True)
                exponent = jnp.exp(scores - highest)
                total = jnp.sum(exponent, axis=-1, keepdims=True)
                probabilities = (exponent * (1.0 / total)).astype(jnp.bfloat16)
                result = jnp.dot(
                    probabilities.reshape(group * rows, seen),
                    vs[slot0 + s, g, :seen, :],
                    preferred_element_type=jnp.float32,
                ).astype(jnp.bfloat16)
                for e in range(group):
                    head = g * group + e
                    mixed[s * rows : (s + 1) * rows, head * HD : (head + 1) * HD] = result[
                        e * rows : (e + 1) * rows
                    ]

    for table in tables:
        table.wait()
    x_copy.wait()
    normalise(0, 0, length, 0)
    sib_copy.wait_recv()
    normalise(1, 0, length, length)
    project(0, 0, length, True)
    attention(0, 0, length, mixed_own)

    for h in range(HALVES):
        row0 = h * part
        far_copy(h).wait_recv()
        fwd_copy(h).start()
        normalise(2, row0, part, 0)
        fwd_copy(h).wait_recv()
        normalise(3, row0, part, part)
        project(2, row0, part, False)
        attention(2, row0, part, mixed_far)

        def far_out(j, carry, h=h):
            @pl.when(j < OUT_TILES)
            def _():
                if h == 0:
                    w2_copy(j).wait()
                partial = jnp.dot(mixed_far[...], w2[j], preferred_element_type=jnp.float32)
                held[j] = partial[:part]
                give[h, j] = partial[part:].astype(jnp.bfloat16)
                give_copy(h, j).start()

            @pl.when(j >= LAG)
            def _():
                t = j - LAG
                give_copy(h, t).wait_recv()
                summed[h, t] = (held[t] + got[h, t].astype(jnp.float32)).astype(jnp.bfloat16)
                sum_copy(h, t).start()

            return carry

        lax.fori_loop(0, OUT_TILES + LAG, far_out, 0)

    def own_out(j, carry):
        partial = jnp.dot(mixed_own[...], w2[j], preferred_element_type=jnp.float32)
        own_acc[j] = partial[:length]
        own_give[j] = partial[length:].astype(jnp.bfloat16)
        own_copy(j).start()
        return carry

    lax.fori_loop(0, OUT_TILES, own_out, 0)

    for h in range(HALVES):

        def finish(j, carry, h=h):
            rows = pl.ds(h * part, part)
            if h == 0:
                own_copy(j).wait_recv()
            sum_copy(h, j).wait_recv()
            cols = pl.ds(pl.multiple_of(j * o_width, o_width), o_width)
            out[0, rows, cols] = (
                own_acc[j, rows, :] + own_got[j, rows, :].astype(jnp.float32)
                + landed[h, j].astype(jnp.float32)
            ).astype(jnp.bfloat16)
            return carry

        lax.fori_loop(0, OUT_TILES, finish, 0)

    def drain(j, carry):
        own_copy(j).wait_send()
        for h in range(HALVES):
            give_copy(h, j).wait_send()
            sum_copy(h, j).wait_send()
        return carry

    lax.fori_loop(0, OUT_TILES, drain, 0)
    sib_copy.wait_send()
    for h in range(HALVES):
        far_copy(h).wait_send()
        fwd_copy(h).wait_send()


def paired_shards(hidden_in, norm_gain, query_weight, kv_weight, output_weight):
    _, length, width = hidden_in.shape
    query_cols, kv_cols = query_weight.shape[1], kv_weight.shape[1]
    heads, kvh = query_cols // HD, kv_cols // (2 * HD)
    q_tiles = query_cols // (2 * HD)
    part = length // HALVES
    o_width = width // OUT_TILES
    cosine, sine = rotary_tables(length)
    bf16, f32 = jnp.bfloat16, jnp.float32
    dma = pltpu.SemaphoreType.DMA
    any_spec = pl.BlockSpec(memory_space=pl.ANY)
    dims = (length, kvh, heads // kvh, q_tiles, o_width)
    return pl.pallas_call(
        functools.partial(block_kernel, dims),
        out_shape=pltpu.VMEM(hidden_in.shape, bf16),
        in_specs=[any_spec] * 7,
        out_specs=pl.BlockSpec(memory_space=pltpu.VMEM),
        scratch_shapes=[
            pltpu.VMEM((1, width), f32),
            pltpu.VMEM((length, HD), f32),
            pltpu.VMEM((length, HD), f32),
            pltpu.VMEM((4, length, width), bf16),
            pltpu.VMEM((2 * length, width), bf16),
            pltpu.VMEM((kvh + q_tiles, width, 2 * HD), bf16),
            pltpu.VMEM((OUT_TILES, query_cols, o_width), bf16),
            pltpu.VMEM((2, heads, length, HD), bf16),
            pltpu.VMEM((4, kvh, length, HD), bf16),
            pltpu.VMEM((4, kvh, length, HD), bf16),
            pltpu.VMEM((2 * length, query_cols), bf16),
            pltpu.VMEM((2 * part, query_cols), bf16),
            pltpu.VMEM((HALVES, OUT_TILES, part, o_width), bf16),
            pltpu.VMEM((HALVES, OUT_TILES, part, o_width), bf16),
            pltpu.VMEM((OUT_TILES, part, o_width), f32),
            pltpu.VMEM((HALVES, OUT_TILES, part, o_width), bf16),
            pltpu.VMEM((HALVES, OUT_TILES, part, o_width), bf16),
            pltpu.VMEM((OUT_TILES, length, o_width), f32),
            pltpu.VMEM((OUT_TILES, length, o_width), bf16),
            pltpu.VMEM((OUT_TILES, length, o_width), bf16),
            dma,
            dma((kvh + q_tiles,)),
            dma((OUT_TILES,)),
            dma, dma,
            dma((HALVES,)), dma((HALVES,)),
            dma((HALVES,)), dma((HALVES,)),
            dma((HALVES, OUT_TILES)), dma((HALVES, OUT_TILES)),
            dma((HALVES, OUT_TILES)), dma((HALVES, OUT_TILES)),
            dma((OUT_TILES,)), dma((OUT_TILES,)),
            dma((3,)),
        ],
        compiler_params=pltpu.CompilerParams(
            collective_id=0, has_side_effects=True, vmem_limit_bytes=60 * 2**20
        ),
    )(
        hidden_in, norm_gain.reshape(1, width), query_weight, kv_weight, output_weight,
        jnp.asarray(cosine), jnp.asarray(sine),
    )


def shards(hidden_in, norm_gain, query_weight, kv_weight, output_weight):
    two_chips = lax.axis_size("tensor") == 2 * CORES
    whole_heads = kv_weight.shape[1] % (2 * HD) == 0
    if two_chips and whole_heads and hidden_in.shape[0] == 1:
        return paired_shards(hidden_in, norm_gain, query_weight, kv_weight, output_weight)
    return general_shards(hidden_in, norm_gain, query_weight, kv_weight, output_weight)


def solution(mesh):
    placed = (
        P(("dp", "tensor"), None, None),
        P(),
        P(None, "tensor"),
        P(None, "tensor"),
        P("tensor", None),
    )
    return jax.shard_map(
        shards,
        mesh=mesh,
        in_specs=placed,
        out_specs=P(("dp", "tensor"), None, None),
        check_vma=False,
    )
```
